32 devices in a mesh: dp: 1 (over z), tp: 4 (over y), ep: 8 (over x, core).
Axes of the slice: x: 4, y: 4, z: 1, core: 2. Of those that a mesh axis runs over, the one named last changes fastest.
The devices are a block of a 4x4x8 slice.
Arguments:
- x: bfloat16 [2048, 2048], P(('dp', 'ep', 'tp'))
- idx: int32 [2048, 6], P(('dp', 'ep', 'tp'))
- gate: float32 [2048, 6], P(('dp', 'ep', 'tp'))
- w1: bfloat16 [64, 2048, 1408], P('ep', None, 'tp')
- w3: bfloat16 [64, 2048, 1408], P('ep', None, 'tp')
- w2: bfloat16 [64, 1408, 2048], P('ep', 'tp')
Outputs:
- output: bfloat16 [2048, 2048], P(('dp', 'ep', 'tp'))
All inputs are finite; a program needn't handle non-finite values.
Results may differ from the reference program's by a relative error of at most 0.001.
Values are sent between devices in bfloat16 or wider.
A program may use at most 768 MiB of HBM per device.

```python
import jax
import jax.numpy as jnp
from jax import lax

D = 2048
FF = 1408
EXPERTS = 64
TOP = 6
TOKENS_DEV = 64
EP = 8
TP = 4

ROWS = TOKENS_DEV * EP * TP
CAP = 8 * ((TOP * ROWS // EXPERTS + 9) // 8)


def _route(key):
    ndev = EP * TP
    nb = TOKENS_DEV // EP
    m = EXPERTS // EP
    k1 = (TOP + 1) // 2
    k2 = TOP - k1
    ka, kd, kt1, kt2, ks = jax.random.split(key, 5)
    a = jnp.argsort(jax.random.uniform(ka, (ndev, nb, EP)), axis=-1).astype(jnp.int32)
    shift = jax.random.randint(kd, (ndev, nb, 1), 1, EP)
    b = (a + shift) % EP
    r = (jnp.arange(ndev)[:, None] * nb + jnp.arange(nb)[None, :])[:, :, None]
    tau1 = jax.random.randint(kt1, (EP,), 0, m)
    tau2 = jax.random.randint(kt2, (EP,), 0, m)
    c1 = (r * k1 + tau1[a]) % m
    c2 = (r * k2 + tau2[b]) % m
    e1 = a[..., None] * m + (c1[..., None] + jnp.arange(k1)) % m
    e2 = b[..., None] * m + (c2[..., None] + jnp.arange(k2)) % m
    idx = jnp.concatenate([e1, e2], axis=-1).reshape(ROWS, TOP)
    perm = jnp.argsort(jax.random.uniform(ks, (ROWS, TOP)), axis=-1)
    return jnp.take_along_axis(idx, perm, axis=1).astype(jnp.int32)


def _weights(key, shape, fan_in):
    keys = jax.random.split(key, EXPERTS)
    return lax.map(lambda k: (jax.random.normal(k, shape, jnp.float32) * fan_in ** -0.5).astype(jnp.bfloat16), keys)


def setup_inputs(seed: int = 0, part: int = 0) -> dict:
    key = jax.random.PRNGKey(seed)
    k_shared, k_part = jax.random.split(key)
    kx, kr, kg = jax.random.split(jax.random.fold_in(k_part, part), 3)
    k1, k3, k2 = jax.random.split(k_shared, 3)
    x = jax.random.normal(kx, (ROWS, D), jnp.float32).astype(jnp.bfloat16)
    idx = _route(kr)
    gate = jax.nn.softmax(0.5 * jax.random.normal(kg, (ROWS, TOP), jnp.float32), axis=-1)
    return {'x': x, 'idx': idx, 'gate': gate,
            'w1': _weights(k1, (D, FF), D), 'w3': _weights(k3, (D, FF), D), 'w2': _weights(k2, (FF, D), FF)}


def reference(x, idx, gate, w1, w3, w2):
    flat = idx.reshape(-1)
    gflat = gate.reshape(-1)
    order = jnp.argsort(flat)
    counts = jnp.zeros((EXPERTS,), jnp.int32).at[flat].add(1)
    starts = jnp.cumsum(counts) - counts
    slot = jnp.arange(CAP)

    def body(acc, e_in):
        w1e, w3e, w2e, start, count = e_in
        pid = order[jnp.clip(start + slot, 0, flat.shape[0] - 1)]
        tok = pid // TOP
        g = jnp.where(slot < count, gflat[pid], 0.0)
        xe = x[tok]
        a = jnp.dot(xe, w1e, preferred_element_type=jnp.float32)
        b = jnp.dot(xe, w3e, preferred_element_type=jnp.float32)
        h = (jax.nn.silu(a) * b).astype(jnp.bfloat16)
        o = jnp.dot(h, w2e, preferred_element_type=jnp.float32)
        return acc.at[tok].add(o * g[:, None]), None

    acc, _ = lax.scan(body, jnp.zeros((ROWS, D), jnp.float32), (w1, w3, w2, starts, counts))
    return acc.astype(jnp.bfloat16)
```

```python
import functools

import jax
import jax.numpy as jnp
from jax import lax
from jax.experimental import pallas as pl
from jax.experimental.pallas import tpu as pltpu
from jax.sharding import PartitionSpec as P

MESH = pl.DeviceIdType.MESH
F32, BF16 = jnp.float32, jnp.bfloat16
META = 128
COLS = 512


def _kernel(n_ep, x_ref, idx_ref, gate_ref, w1_hbm, w3_hbm, w2_hbm, y_ref,
            st, send, xr, w1, w3, w2, hid, gat, part, near, full, back,
            w_sem, xs, xv, ys, yv, fs, fv, ns, nv, us, uv, bs, bv):
    rows, width = x_ref.shape
    top = idx_ref.shape[1]
    n_exp = w1.shape[0]
    blk = 2 * rows // n_ep
    half_ep = n_ep // 2
    kl_n = n_ep // 2
    via = kl_n // 2
    vrows = kl_n * blk
    crows = 4 * vrows
    n_col = width // COLS

    p, t = lax.axis_index('ep'), lax.axis_index('tp')
    cx, cc = p // 2, p % 2
    up, dn = {'tp': (t + 1) % 4}, {'tp': (t + 3) % 4}

    def dest(k):
        return {'ep': 2 * ((cx + half_ep - k // 2) % half_ep) + (cc + k % 2) % 2}

    def home(k):
        return {'ep': 2 * ((cx + k // 2) % half_ep) + (cc + k % 2) % 2}

    def place(k, v):
        return pl.ds((k // kl_n) * crows + v * vrows + (k % kl_n) * blk, blk)

    def remote(src, dst, s, r, dev):
        return pltpu.make_async_remote_copy(src_ref=src, dst_ref=dst, send_sem=s, recv_sem=r,
                                            device_id=dev, device_id_type=MESH)

    def weights(e):
        return [pltpu.make_async_copy(h.at[e], v.at[e], w_sem.at[i, e])
                for i, (h, v) in enumerate(((w1_hbm, w1), (w3_hbm, w3), (w2_hbm, w2)))]

    for e in range(n_exp):
        for c in weights(e)[:2]:
            c.start()
    for e in range(n_exp):
        weights(e)[2].start()

    barrier = pltpu.get_barrier_semaphore()
    for k in range(1, n_ep):
        pl.semaphore_signal(barrier, inc=1, device_id=dest(k), device_id_type=MESH)
    pl.semaphore_signal(barrier, inc=1, device_id=up, device_id_type=MESH)
    pl.semaphore_signal(barrier, inc=1, device_id=dn, device_id_type=MESH)

    idx = idx_ref[...]
    gate = gate_ref[...]
    lanes = n_ep * blk
    lane = lax.broadcasted_iota(jnp.int32, (rows, lanes), 1)
    kk = lax.div(lane, blk)
    pos_of = 2 * lax.rem(cx + half_ep - lax.div(kk, 2), half_ep) + lax.rem(cc + lax.rem(kk, 2), 2)
    first = pos_of * n_exp
    hit = jnp.zeros((rows, lanes), F32)
    for j in range(top):
        col = idx[:, j:j + 1]
        hit = jnp.where((col >= first) & (col < first + n_exp), 1.0, hit)
    lower = jnp.where(lax.broadcasted_iota(jnp.int32, (rows, rows), 0) > lax.broadcasted_iota(jnp.int32, (rows, rows), 1),
                      1.0, 0.0)
    rank = jnp.dot(lower.astype(BF16), hit.astype(BF16), preferred_element_type=F32)
    sel = jnp.where((rank == lax.rem(lane, blk).astype(F32)), hit, 0.0)
    st[...] = sel
    pick = sel.T.astype(BF16)

    mlane = lax.broadcasted_iota(jnp.int32, (rows, META), 1)
    g_hi = gate.astype(BF16).astype(F32)
    g_mid = (gate - g_hi).astype(BF16).astype(F32)
    g_lo = gate - g_hi - g_mid
    meta = jnp.full((rows, META), -1.0, F32)
    for j in range(top):
        meta = jnp.where(mlane == j, idx[:, j:j + 1].astype(F32), meta)
        meta = jnp.where(mlane == 8 + j, g_hi[:, j:j + 1], meta)
        meta = jnp.where(mlane == 16 + j, g_mid[:, j:j + 1], meta)
        meta = jnp.where(mlane == 24 + j, g_lo[:, j:j + 1], meta)
    sent_meta = jnp.dot(pick, meta.astype(BF16), preferred_element_type=F32).astype(BF16)
    sent = jnp.dot(pick, x_ref[...], preferred_element_type=F32).astype(BF16)
    xr[:blk, :width] = sent[:blk]
    xr[:blk, width:] = sent_meta[:blk]
    send[:, :width] = sent
    send[:, width:] = sent_meta

    pl.semaphore_wait(barrier, n_ep + 1)

    def to_pos(k):
        return remote(send.at[pl.ds(k * blk, blk)], xr.at[place(k, 0)], xs.at[k], xv.at[k], dest(k))

    def spread(k):
        own = xr.at[place(k, 0)]
        return (remote(own, xr.at[place(k, 3)], ys.at[k, 0], yv.at[k, 0], up),
                remote(own, xr.at[place(k, 1)], ys.at[k, 1], yv.at[k, 1], dn))

    def forward(k):
        if k % kl_n < via:
            return remote(xr.at[place(k, 3)], xr.at[place(k, 2)], fs.at[k], fv.at[k], up)
        return remote(xr.at[place(k, 1)], xr.at[place(k, 2)], fs.at[k], fv.at[k], dn)

    def start_spread(k):
        if k:
            to_pos(k).wait_recv()
        for c in spread(k):
            c.start()

    def start_forward(k):
        spread(k)[0 if k % kl_n < via else 1].wait_recv()
        forward(k).start()

    start_spread(0)
    for k in range(1, n_ep):
        to_pos(k).start()
    for k in range(1, kl_n):
        start_spread(k)
        start_forward(k - 1)
    start_forward(kl_n - 1)
    for k in range(kl_n, n_ep):
        start_spread(k)

    half = via * blk

    def opposite(c, n):
        return (remote(part.at[c, n, pl.ds(2 * vrows, half)], near.at[c, n, 0], ns.at[c, n, 0], nv.at[c, n, 0], up),
                remote(part.at[c, n, pl.ds(2 * vrows + half, vrows - half)], near.at[c, n, 1], ns.at[c, n, 1], nv.at[c, n, 1], dn))

    def beside(c, n):
        return (remote(part.at[c, n, pl.ds(vrows, vrows)], full.at[c, n, 0], us.at[c, n, 0], uv.at[c, n, 0], up),
                remote(part.at[c, n, pl.ds(3 * vrows, vrows)], full.at[c, n, 1], us.at[c, n, 1], uv.at[c, n, 1], dn))

    def homeward(k, n):
        return remote(part.at[k // kl_n, n, pl.ds((k % kl_n) * blk, blk)], back.at[n, pl.ds(k * blk, blk)],
                      bs.at[k, n], bv.at[k, n], home(k))

    def start_beside(c, n):
        for r in opposite(c, n):
            r.wait_recv()
        part[c, n, pl.ds(vrows, half)] += near[c, n, 0]
        part[c, n, pl.ds(3 * vrows + half, vrows - half)] += near[c, n, 1]
        for r in beside(c, n):
            r.start()

    def start_homeward(c, n):
        for r in beside(c, n):
            r.wait_recv()
        total = part[c, n, pl.ds(0, vrows)] + full[c, n, 0] + full[c, n, 1]
        part[c, n, pl.ds(0, vrows)] = total
        if c == 0:
            back[n, pl.ds(0, blk)] = total[:blk]
        for k in range(max(c * kl_n, 1), (c + 1) * kl_n):
            homeward(k, n).start()

    for c in range(2):
        for k in range(c * kl_n, (c + 1) * kl_n):
            spread(k)[1 if k % kl_n < via else 0].wait_recv()
            forward(k).wait_recv()

        base = c * crows
        m = xr[pl.ds(base, crows), width:].astype(F32)
        g_sum = m + pltpu.roll(m, META - 8, 1) + pltpu.roll(m, META - 16, 1)
        el = (lax.broadcasted_iota(jnp.int32, (crows, META), 1) + p * n_exp).astype(F32)
        g = jnp.zeros((crows, META), F32)
        for j in range(top):
            g = g + jnp.where(m[:, j:j + 1] == el, g_sum[:, 8 + j:9 + j], 0.0)
        gat[...] = g

        def hidden(e, carry, c=c, base=base):
            if c == 0:
                for w in weights(e)[:2]:
                    w.wait()
                for kl in range(kl_n):
                    @pl.when(e == n_exp - kl_n + kl)
                    def _():
                        start_forward(kl_n + kl)
            else:
                for n in range(n_col):
                    @pl.when(e == n_exp - 2 * n_col + 2 * n + 1)
                    def _():
                        start_beside(0, n)
            xc = xr[pl.ds(base, crows), :width]
            a = jnp.dot(xc, w1[e], preferred_element_type=F32)
            b = jnp.dot(xc, w3[e], preferred_element_type=F32)
            hid[e] = (a * jax.nn.sigmoid(a) * b).astype(BF16)
            return carry

        lax.fori_loop(0, n_exp, hidden, 0)
        if c == 0:
            for e in range(n_exp):
                weights(e)[2].wait()

        def outputs(n, carry, c=c):
            acc = None
            cols = pl.ds(pl.multiple_of(n * COLS, COLS), COLS)
            for e in range(n_exp):
                o = jnp.dot(hid[e], w2[e, :, cols], preferred_element_type=F32) * gat[:, e:e + 1]
                acc = o if acc is None else acc + o
            part[c, n] = acc
            for r in opposite(c, n):
                r.start()
            if c == 1:
                start_homeward(0, n)
            return carry

        lax.fori_loop(0, n_col, outputs, 0)

    for n in range(n_col):
        start_beside(1, n)
    for n in range(n_col):
        start_homeward(1, n)
    for n in range(n_col):
        for k in range(1, n_ep):
            homeward(k, n).wait_recv()
        y_ref[:, n * COLS:(n + 1) * COLS] = jnp.dot(
            st[...], back[n], precision=lax.Precision.HIGHEST, preferred_element_type=F32).astype(BF16)

    for k in range(n_ep):
        if k:
            to_pos(k).wait_send()
        for c in spread(k):
            c.wait_send()
        forward(k).wait_send()
        if k:
            for n in range(n_col):
                homeward(k, n).wait_send()
    for c in range(2):
        for n in range(n_col):
            for r in opposite(c, n) + beside(c, n):
                r.wait_send()


def solution(mesh):
    n_ep = mesh.shape['ep']
    rows_spec = P(('dp', 'ep', 'tp'), None)

    def body(x, idx, gate, w1, w3, w2):
        rows, width = x.shape
        n_exp, _, ff = w1.shape
        blk = 2 * rows // n_ep
        kl_n = n_ep // 2
        vrows, crows, n_col = kl_n * blk, 4 * kl_n * blk, width // COLS
        half = kl_n // 2 * blk
        dma = pltpu.SemaphoreType.DMA
        vmem = pl.BlockSpec(memory_space=pltpu.VMEM)
        anyw = pl.BlockSpec(memory_space=pl.ANY)
        return pl.pallas_call(
            functools.partial(_kernel, n_ep),
            out_shape=jax.ShapeDtypeStruct((rows, width), BF16),
            in_specs=[vmem] * 3 + [anyw] * 3,
            out_specs=vmem,
            scratch_shapes=[
                pltpu.VMEM((rows, n_ep * blk), F32),
                pltpu.VMEM((n_ep * blk, width + META), BF16),
                pltpu.VMEM((2 * crows, width + META), BF16),
                pltpu.VMEM(w1.shape, BF16),
                pltpu.VMEM(w3.shape, BF16),
                pltpu.VMEM(w2.shape, BF16),
                pltpu.VMEM((n_exp, crows, ff), BF16),
                pltpu.VMEM((crows, META), F32),
                pltpu.VMEM((2, n_col, crows, COLS), F32),
                pltpu.VMEM((2, n_col, 2, half, COLS), F32),
                pltpu.VMEM((2, n_col, 2, vrows, COLS), F32),
                pltpu.VMEM((n_col, n_ep * blk, COLS), F32),
                dma((3, n_exp)),
                dma((n_ep,)), dma((n_ep,)),
                dma((n_ep, 2)), dma((n_ep, 2)),
                dma((n_ep,)), dma((n_ep,)),
                dma((2, n_col, 2)), dma((2, n_col, 2)),
                dma((2, n_col, 2)), dma((2, n_col, 2)),
                dma((n_ep, n_col)), dma((n_ep, n_col)),
            ],
            compiler_params=pltpu.CompilerParams(
                collective_id=0, has_side_effects=True, vmem_limit_bytes=63 * 1024 * 1024),
        )(x, idx, gate, w1, w3, w2)

    return jax.shard_map(body, mesh=mesh,
                         in_specs=(rows_spec, rows_spec, rows_spec,
                                   P('ep', None, 'tp'), P('ep', None, 'tp'), P('ep', 'tp', None)),
                         out_specs=rows_spec, check_vma=False)
```

```python
import functools

import jax
import jax.numpy as jnp
from jax import lax
from jax.experimental import pallas as pl
from jax.experimental.pallas import tpu as pltpu
from jax.sharding import PartitionSpec as P

MESH = pl.DeviceIdType.MESH
F32, BF16 = jnp.float32, jnp.bfloat16
META = 128
COLS = 512


def _kernel(n_ep, x_ref, idx_ref, gate_ref, w1_hbm, w3_hbm, w2_hbm, y_ref,
            st, mt, send, xr, w13, w2, hid, gat, part, near, full, back,
            w_sem, xs, xv, ys, yv, fs, fv, ns, nv, us, uv, bs, bv):
    rows, width = x_ref.shape
    top = idx_ref.shape[0]
    n_exp, ff, _ = w2.shape
    main = ff // 256 * 256
    rest = -(-(ff - main) // 128) * 128
    pad = main + rest - ff
    blk = 2 * rows // n_ep
    half_ep = n_ep // 2
    kl_n = n_ep // 2
    via = kl_n // 2
    vrows = kl_n * blk
    crows = 4 * vrows
    n_col = width // COLS

    p, t = lax.axis_index('ep'), lax.axis_index('tp')
    cx, cc = p // 2, p % 2
    up, dn = {'tp': (t + 1) % 4}, {'tp': (t + 3) % 4}

    def dest(k):
        return {'ep': 2 * ((cx + half_ep - k // 2) % half_ep) + (cc + k % 2) % 2}

    def home(k):
        return {'ep': 2 * ((cx + k // 2) % half_ep) + (cc + k % 2) % 2}

    def place(k, v):
        return pl.ds((k // kl_n) * crows + v * vrows + (k % kl_n) * blk, blk)

    def remote(src, dst, s, r, dev):
        return pltpu.make_async_remote_copy(src_ref=src, dst_ref=dst, send_sem=s, recv_sem=r,
                                            device_id=dev, device_id_type=MESH)

    def up_weights(e):
        parts = []
        for i, h in enumerate((w1_hbm, w3_hbm)):
            if main:
                parts.append((h.at[e, pl.ds(0, main)], w13.at[e, pl.ds(i * main, main)], w_sem.at[2 * i, e]))
            if rest:
                parts.append((h.at[e, pl.ds(main, ff - main)], w13.at[e, pl.ds(2 * main + i * rest, ff - main)],
                              w_sem.at[2 * i + 1, e]))
        return [pltpu.make_async_copy(*q) for q in parts]

    def down_weights(e):
        return pltpu.make_async_copy(w2_hbm.at[e], w2.at[e], w_sem.at[4, e])

    for e in range(n_exp):
        for c in up_weights(e):
            c.start()
    for e in range(n_exp):
        down_weights(e).start()

    barrier = pltpu.get_barrier_semaphore()
    for k in range(1, n_ep):
        pl.semaphore_signal(barrier, inc=1, device_id=dest(k), device_id_type=MESH)
    pl.semaphore_signal(barrier, inc=1, device_id=up, device_id_type=MESH)
    pl.semaphore_signal(barrier, inc=1, device_id=dn, device_id_type=MESH)

    idx = idx_ref[...]
    gate = gate_ref[...]
    lanes = n_ep * blk
    slot = lax.broadcasted_iota(jnp.int32, (lanes, rows), 0)
    kk = lax.div(slot, blk)
    pos_of = 2 * lax.rem(cx + half_ep - lax.div(kk, 2), half_ep) + lax.rem(cc + lax.rem(kk, 2), 2)
    first = pos_of * n_exp
    hit = jnp.zeros((lanes, rows), F32)
    for j in range(top):
        row = idx[j:j + 1]
        hit = jnp.where((row >= first) & (row < first + n_exp), 1.0, hit)
    before = jnp.where(lax.broadcasted_iota(jnp.int32, (rows, rows), 0) < lax.broadcasted_iota(jnp.int32, (rows, rows), 1),
                       1.0, 0.0)
    rank = jnp.dot(hit.astype(BF16), before.astype(BF16), preferred_element_type=F32)
    sel = jnp.where(rank == lax.rem(slot, blk).astype(F32), hit, 0.0)
    pick = sel.astype(BF16)

    g_hi = gate.astype(BF16).astype(F32)
    g_mid = (gate - g_hi).astype(BF16).astype(F32)
    mt[...] = jnp.zeros_like(mt)
    mt[0:top] = idx.astype(F32)
    mt[8:8 + top] = g_hi
    mt[16:16 + top] = g_mid
    mt[24:24 + top] = gate - g_hi - g_mid
    sent_meta = lax.dot_general(pick, mt[...].astype(BF16), (((1,), (1,)), ((), ())),
                                preferred_element_type=F32).astype(BF16)
    sent = jnp.dot(pick, x_ref[...], preferred_element_type=F32).astype(BF16)
    xr[:blk, :width] = sent[:blk]
    xr[:blk, width:] = sent_meta[:blk]
    send[:, :width] = sent
    send[:, width:] = sent_meta

    pl.semaphore_wait(barrier, n_ep + 1)

    def to_pos(k):
        return remote(send.at[pl.ds(k * blk, blk)], xr.at[place(k, 0)], xs.at[k], xv.at[k], dest(k))

    def spread(k, i):
        return remote(xr.at[place(k, 0)], xr.at[place(k, 1 if i else 3)], ys.at[k, i], yv.at[k, i], dn if i else up)

    def way(k):
        return 0 if k % kl_n < via else 1

    def forward(k):
        return remote(xr.at[place(k, 1 if way(k) else 3)], xr.at[place(k, 2)], fs.at[k], fv.at[k], dn if way(k) else up)

    def start_spread(k):
        if k:
            to_pos(k).wait_recv()
        spread(k, 0).start()
        spread(k, 1).start()

    def start_forward(k):
        spread(k, way(k)).wait_recv()
        forward(k).start()

    start_spread(0)
    for k in range(1, n_ep):
        to_pos(k).start()
    for k in range(1, kl_n):
        start_spread(k)
        start_forward(k - 1)
    start_forward(kl_n - 1)
    for k in range(kl_n, n_ep):
        start_spread(k)
    st[...] = sel.T
    if pad:
        for i in range(2):
            w13[:, pl.ds(2 * main + i * rest + rest - pad, pad)] = jnp.zeros((n_exp, pad, width), BF16)

    half = via * blk

    def opposite(c, n):
        return (remote(part.at[c, n, pl.ds(2 * vrows, half)], near.at[c, n, 0], ns.at[c, n, 0], nv.at[c, n, 0], up),
                remote(part.at[c, n, pl.ds(2 * vrows + half, vrows - half)], near.at[c, n, 1], ns.at[c, n, 1], nv.at[c, n, 1], dn))

    def beside(c, n):
        return (remote(part.at[c, n, pl.ds(vrows, vrows)], full.at[c, n, 0], us.at[c, n, 0], uv.at[c, n, 0], up),
                remote(part.at[c, n, pl.ds(3 * vrows, vrows)], full.at[c, n, 1], us.at[c, n, 1], uv.at[c, n, 1], dn))

    def homeward(k, n):
        return remote(part.at[k // kl_n, n, pl.ds((k % kl_n) * blk, blk)], back.at[n, pl.ds(k * blk, blk)],
                      bs.at[k, n], bv.at[k, n], home(k))

    def start_beside(c, n):
        for r in opposite(c, n):
            r.wait_recv()
        part[c, n, pl.ds(vrows, half)] += near[c, n, 0]
        part[c, n, pl.ds(3 * vrows + half, vrows - half)] += near[c, n, 1]
        for r in beside(c, n):
            r.start()

    def start_homeward(c, n):
        for r in beside(c, n):
            r.wait_recv()
        total = part[c, n, pl.ds(0, vrows)] + full[c, n, 0] + full[c, n, 1]
        part[c, n, pl.ds(0, vrows)] = total
        if c == 0:
            back[n, pl.ds(0, blk)] = total[:blk]
        for k in range(max(c * kl_n, 1), (c + 1) * kl_n):
            homeward(k, n).start()

    for c in range(2):
        for k in range(c * kl_n, (c + 1) * kl_n):
            spread(k, 1 - way(k)).wait_recv()
            forward(k).wait_recv()

        base = c * crows
        m = xr[pl.ds(base, crows), width:].astype(F32)
        g_sum = m + pltpu.roll(m, META - 8, 1) + pltpu.roll(m, META - 16, 1)
        el = (lax.broadcasted_iota(jnp.int32, (crows, META), 1) + p * n_exp).astype(F32)
        g = jnp.zeros((crows, META), F32)
        for j in range(top):
            g = g + jnp.where(m[:, j:j + 1] == el, g_sum[:, 8 + j:9 + j], 0.0)
        gat[...] = g

        def hidden(e, carry, c=c, base=base):
            if c == 0:
                for w in up_weights(e):
                    w.wait()
                for kl in range(kl_n):
                    @pl.when(e == n_exp - kl_n + kl)
                    def _():
                        start_forward(kl_n + kl)
            else:
                for n in range(n_col):
                    @pl.when(e == n_exp - 2 * n_col + 2 * n + 1)
                    def _():
                        start_beside(0, n)
            xc = xr[pl.ds(base, crows), :width]
            ab = lax.dot_general(xc, w13[e], (((1,), (1,)), ((), ())), preferred_element_type=F32)
            for at, n in ((0, main), (2 * main, rest)):
                if n:
                    a, b = ab[:, at:at + n], ab[:, at + n:at + 2 * n]
                    hid[e, :, at // 2:at // 2 + n] = (a * jax.nn.sigmoid(a) * b).astype(BF16)
            return carry

        lax.fori_loop(0, n_exp, hidden, 0)
        if c == 0:
            for e in range(n_exp):
                down_weights(e).wait()

        def outputs(n, carry, c=c):
            acc = None
            cols = pl.ds(pl.multiple_of(n * COLS, COLS), COLS)
            for e in range(n_exp):
                o = jnp.dot(hid[e, :, :ff], w2[e, :, cols], preferred_element_type=F32) * gat[:, e:e + 1]
                acc = o if acc is None else acc + o
            part[c, n] = acc
            for r in opposite(c, n):
                r.start()
            if c == 1:
                start_homeward(0, n)
            return carry

        lax.fori_loop(0, n_col, outputs, 0)

    for n in range(n_col):
        start_beside(1, n)
    for n in range(n_col):
        start_homeward(1, n)
    for n in range(n_col):
        for k in range(1, n_ep):
            homeward(k, n).wait_recv()
        y_ref[:, n * COLS:(n + 1) * COLS] = jnp.dot(
            st[...], back[n], precision=lax.Precision.HIGHEST, preferred_element_type=F32).astype(BF16)

    for k in range(n_ep):
        if k:
            to_pos(k).wait_send()
        spread(k, 0).wait_send()
        spread(k, 1).wait_send()
        forward(k).wait_send()
        if k:
            for n in range(n_col):
                homeward(k, n).wait_send()
    for c in range(2):
        for n in range(n_col):
            for r in opposite(c, n) + beside(c, n):
                r.wait_send()


def solution(mesh):
    n_ep = mesh.shape['ep']
    rows_spec = P(('dp', 'ep', 'tp'), None)

    def body(x, idx, gate, w1, w3, w2):
        rows, width = x.shape
        n_exp, _, ff = w1.shape
        wide = ff // 256 * 256 - (-(ff % 256) // 128) * 128
        blk = 2 * rows // n_ep
        kl_n = n_ep // 2
        vrows, crows, n_col = kl_n * blk, 4 * kl_n * blk, width // COLS
        half = kl_n // 2 * blk
        dma = pltpu.SemaphoreType.DMA
        vmem = pl.BlockSpec(memory_space=pltpu.VMEM)
        anyw = pl.BlockSpec(memory_space=pl.ANY)
        return pl.pallas_call(
            functools.partial(_kernel, n_ep),
            out_shape=jax.ShapeDtypeStruct((rows, width), BF16),
            in_specs=[vmem] * 3 + [anyw] * 3,
            out_specs=vmem,
            scratch_shapes=[
                pltpu.VMEM((rows, n_ep * blk), F32),
                pltpu.VMEM((META, rows), F32),
                pltpu.VMEM((n_ep * blk, width + META), BF16),
                pltpu.VMEM((2 * crows, width + META), BF16),
                pltpu.VMEM((n_exp, 2 * wide, width), BF16),
                pltpu.VMEM(w2.shape, BF16),
                pltpu.VMEM((n_exp, crows, wide), BF16),
                pltpu.VMEM((crows, META), F32),
                pltpu.VMEM((2, n_col, crows, COLS), F32),
                pltpu.VMEM((2, n_col, 2, half, COLS), F32),
                pltpu.VMEM((2, n_col, 2, vrows, COLS), F32),
                pltpu.VMEM((n_col, n_ep * blk, COLS), F32),
                dma((5, n_exp)),
                dma((n_ep,)), dma((n_ep,)),
                dma((n_ep, 2)), dma((n_ep, 2)),
                dma((n_ep,)), dma((n_ep,)),
                dma((2, n_col, 2)), dma((2, n_col, 2)),
                dma((2, n_col, 2)), dma((2, n_col, 2)),
                dma((n_ep, n_col)), dma((n_ep, n_col)),
            ],
            compiler_params=pltpu.CompilerParams(
                collective_id=0, has_side_effects=True, vmem_limit_bytes=63 * 1024 * 1024),
        )(x, idx.T, gate.T, w1.swapaxes(1, 2), w3.swapaxes(1, 2), w2)

    return jax.shard_map(body, mesh=mesh,
                         in_specs=(rows_spec, rows_spec, rows_spec,
                                   P('ep', None, 'tp'), P('ep', None, 'tp'), P('ep', 'tp', None)),
                         out_specs=rows_spec, check_vma=False)
```

```python
import functools

import jax
import jax.numpy as jnp
from jax import lax
from jax.experimental import pallas as pl
from jax.experimental.pallas import tpu as pltpu
from jax.sharding import PartitionSpec as P

MESH = pl.DeviceIdType.MESH
F32, BF16, I16 = jnp.float32, jnp.bfloat16, jnp.int16
META = 128
COLS = 512
STEPS = 32767.0
ROUND = 12582912.0


def _column(row, n):
    return jnp.broadcast_to(row, (128, n)).T[:, :1]


def _encode(val):
    n = val.shape[0]
    top = jnp.maximum(jnp.max(jnp.abs(val), axis=1, keepdims=True), 1e-33)
    code = (val * (STEPS / top) + ROUND) - ROUND
    step = jnp.broadcast_to(top * (1.0 / STEPS), (n, 128)).T[:1]
    return code.astype(jnp.int32).astype(jnp.int16), step


def _decode(code, step):
    return code.astype(jnp.int32).astype(F32) * _column(step, code.shape[0])


def _kernel(n_ep, x_ref, idx_ref, gate_ref, w1_hbm, w3_hbm, w2_hbm, y_ref,
            st, mt, send, xr, w13, w2, hid, gat, part, back, back_s,
            far_o, far_os, near, near_s, side_o, side_os, full, full_s, home_o, home_os,
            w_sem, xs, xv, ys, yv, fs, fv, ns, nv, us, uv, bs, bv):
    rows, width = x_ref.shape
    top = idx_ref.shape[0]
    n_exp, ff, _ = w2.shape
    main = ff // 256 * 256
    rest = -(-(ff - main) // 128) * 128
    pad = main + rest - ff
    blk = 2 * rows // n_ep
    half_ep = n_ep // 2
    kl_n = n_ep // 2
    via = kl_n // 2
    vrows = kl_n * blk
    crows = 4 * vrows
    n_col = width // COLS

    p, t = lax.axis_index('ep'), lax.axis_index('tp')
    cx, cc = p // 2, p % 2
    up, dn = {'tp': (t + 1) % 4}, {'tp': (t + 3) % 4}

    def away(q):
        return q if q < 2 else half_ep + 1 - q

    def dest(k):
        return {'ep': 2 * ((cx + half_ep - away(k // 2)) % half_ep) + (cc + k % 2) % 2}

    def home(k):
        return {'ep': 2 * ((cx + away(k // 2)) % half_ep) + (cc + k % 2) % 2}

    def place(k, v):
        return pl.ds((k // kl_n) * crows + v * vrows + (k % kl_n) * blk, blk)

    def remote(src, dst, s, r, dev):
        return pltpu.make_async_remote_copy(src_ref=src, dst_ref=dst, send_sem=s, recv_sem=r,
                                            device_id=dev, device_id_type=MESH)

    def up_weights(e):
        parts = []
        for i, h in enumerate((w1_hbm, w3_hbm)):
            if main:
                parts.append((h.at[e, pl.ds(0, main)], w13.at[e, pl.ds(i * main, main)], w_sem.at[2 * i, e]))
            if rest:
                parts.append((h.at[e, pl.ds(main, ff - main)], w13.at[e, pl.ds(2 * main + i * rest, ff - main)],
                              w_sem.at[2 * i + 1, e]))
        return [pltpu.make_async_copy(*q) for q in parts]

    def down_weights(e):
        return pltpu.make_async_copy(w2_hbm.at[e], w2.at[e], w_sem.at[4, e])

    for e in range(n_exp):
        for c in up_weights(e):
            c.start()
    for e in range(n_exp):
        down_weights(e).start()

    barrier = pltpu.get_barrier_semaphore()
    for k in range(1, n_ep):
        pl.semaphore_signal(barrier, inc=1, device_id=dest(k), device_id_type=MESH)
    pl.semaphore_signal(barrier, inc=1, device_id=up, device_id_type=MESH)
    pl.semaphore_signal(barrier, inc=1, device_id=dn, device_id_type=MESH)

    idx = idx_ref[...]
    gate = gate_ref[...]
    lanes = n_ep * blk
    slot = lax.broadcasted_iota(jnp.int32, (lanes, rows), 0)
    kk = lax.div(slot, blk)
    q = lax.div(kk, 2)
    pos_of = 2 * lax.rem(cx + half_ep - jnp.where(q < 2, q, half_ep + 1 - q), half_ep) + lax.rem(cc + lax.rem(kk, 2), 2)
    first = pos_of * n_exp
    hit = jnp.zeros((lanes, rows), F32)
    for j in range(top):
        row = idx[j:j + 1]
        hit = jnp.where((row >= first) & (row < first + n_exp), 1.0, hit)
    before = jnp.where(lax.broadcasted_iota(jnp.int32, (rows, rows), 0) < lax.broadcasted_iota(jnp.int32, (rows, rows), 1),
                       1.0, 0.0)
    rank = jnp.dot(hit.astype(BF16), before.astype(BF16), preferred_element_type=F32)
    sel = jnp.where(rank == lax.rem(slot, blk).astype(F32), hit, 0.0)
    pick = sel.astype(BF16)

    g_hi = gate.astype(BF16).astype(F32)
    g_mid = (gate - g_hi).astype(BF16).astype(F32)
    mt[...] = jnp.zeros_like(mt)
    mt[0:top] = idx.astype(F32)
    mt[8:8 + top] = g_hi
    mt[16:16 + top] = g_mid
    mt[24:24 + top] = gate - g_hi - g_mid
    sent_meta = lax.dot_general(pick, mt[...].astype(BF16), (((1,), (1,)), ((), ())),
                                preferred_element_type=F32).astype(BF16)
    sent = jnp.dot(pick, x_ref[...], preferred_element_type=F32).astype(BF16)
    xr[:blk, :width] = sent[:blk]
    xr[:blk, width:] = sent_meta[:blk]
    send[:, :width] = sent
    send[:, width:] = sent_meta

    pl.semaphore_wait(barrier, n_ep + 1)

    def to_pos(k):
        return remote(send.at[pl.ds(k * blk, blk)], xr.at[place(k, 0)], xs.at[k], xv.at[k], dest(k))

    def spread(k, i):
        return remote(xr.at[place(k, 0)], xr.at[place(k, 1 if i else 3)], ys.at[k, i], yv.at[k, i], dn if i else up)

    def way(k):
        return 0 if k % kl_n < via else 1

    def forward(k):
        return remote(xr.at[place(k, 1 if way(k) else 3)], xr.at[place(k, 2)], fs.at[k], fv.at[k], dn if way(k) else up)

    def start_spread(k):
        if k:
            to_pos(k).wait_recv()
        spread(k, 0).start()
        spread(k, 1).start()

    def start_forward(k):
        spread(k, way(k)).wait_recv()
        forward(k).start()

    start_spread(0)
    for k in range(1, n_ep):
        to_pos(k).start()
    for k in range(1, kl_n):
        start_spread(k)
        start_forward(k - 1)
    start_forward(kl_n - 1)
    st[...] = sel.T
    if pad:
        for i in range(2):
            w13[:, pl.ds(2 * main + i * rest + rest - pad, pad)] = jnp.zeros((n_exp, pad, width), BF16)

    half = via * blk

    def opposite(c, n):
        out = []
        for i, rows_i, dev in ((0, pl.ds(0, half), up), (1, pl.ds(half, vrows - half), dn)):
            out.append(remote(far_o.at[c, n, rows_i], near.at[c, n, i], ns.at[c, n, i, 0], nv.at[c, n, i, 0], dev))
            out.append(remote(far_os.at[c, n], near_s.at[c, n, i], ns.at[c, n, i, 1], nv.at[c, n, i, 1], dev))
        return out

    def beside(c, n):
        out = []
        for i, dev in ((0, up), (1, dn)):
            out.append(remote(side_o.at[c, n, i], full.at[c, n, i], us.at[c, n, i, 0], uv.at[c, n, i, 0], dev))
            out.append(remote(side_os.at[c, n, i], full_s.at[c, n, i], us.at[c, n, i, 1], uv.at[c, n, i, 1], dev))
        return out

    def homeward(k, n):
        c = k // kl_n
        return [remote(home_o.at[c, n, pl.ds((k % kl_n) * blk, blk)], back.at[n, pl.ds(k * blk, blk)],
                       bs.at[k, n, 0], bv.at[k, n, 0], home(k)),
                remote(home_os.at[c, n], back_s.at[n, k], bs.at[k, n, 1], bv.at[k, n, 1], home(k))]

    def start_opposite(c, n):
        code, step = _encode(part[c, n, pl.ds(2 * vrows, vrows)])
        far_o[c, n] = code
        far_os[c, n] = step
        for r in opposite(c, n):
            r.start()

    def start_beside(c, n):
        for r in opposite(c, n):
            r.wait_recv()
        for i, at in ((0, 0), (1, half)):
            v = (1, 3)[i] * vrows
            size = vrows - half if i else half
            step = near_s[c, n, i][:, at:at + size]
            more = _decode(near[c, n, i], step)
            mine = part[c, n, pl.ds(v, vrows)]
            mine = jnp.concatenate([mine[:half], mine[half:] + more] if i else [mine[:half] + more, mine[half:]], axis=0)
            code, step = _encode(mine)
            side_o[c, n, i] = code
            side_os[c, n, i] = step
        for r in beside(c, n):
            r.start()

    def start_homeward(c, n):
        for r in beside(c, n):
            r.wait_recv()
        total = part[c, n, pl.ds(0, vrows)]
        for i in range(2):
            total = total + _decode(full[c, n, i], full_s[c, n, i])
        code, step = _encode(total)
        home_o[c, n] = code
        home_os[c, n] = step
        if c == 0:
            back[n, pl.ds(0, blk)] = code[:blk]
            back_s[n, 0] = step
        for k in range(max(c * kl_n, 1), (c + 1) * kl_n):
            for r in homeward(k, n):
                r.start()

    for c in range(2):
        for k in range(c * kl_n, (c + 1) * kl_n):
            spread(k, 1 - way(k)).wait_recv()
            forward(k).wait_recv()

        base = c * crows
        m = xr[pl.ds(base, crows), width:].astype(F32)
        g_sum = m + pltpu.roll(m, META - 8, 1) + pltpu.roll(m, META - 16, 1)
        el = (lax.broadcasted_iota(jnp.int32, (crows, META), 1) + p * n_exp).astype(F32)
        g = jnp.zeros((crows, META), F32)
        for j in range(top):
            g = g + jnp.where(m[:, j:j + 1] == el, g_sum[:, 8 + j:9 + j], 0.0)
        gat[...] = g

        def hidden(e, carry, c=c, base=base):
            if c == 0:
                for w in up_weights(e):
                    w.wait()
                for kl in range(kl_n):
                    @pl.when(e == n_exp - 2 * kl_n + kl)
                    def _():
                        start_spread(kl_n + kl)

                    @pl.when(e == n_exp - kl_n + kl)
                    def _():
                        start_forward(kl_n + kl)
            else:
                for n in range(n_col):
                    @pl.when(e == n_exp - 2 * n_col + 2 * n + 1)
                    def _():
                        start_beside(0, n)
            xc = xr[pl.ds(base, crows), :width]
            ab = lax.dot_general(xc, w13[e], (((1,), (1,)), ((), ())), preferred_element_type=F32)
            for at, n in ((0, main), (2 * main, rest)):
                if n:
                    a, b = ab[:, at:at + n], ab[:, at + n:at + 2 * n]
                    hid[e, :, at // 2:at // 2 + n] = (a * jax.nn.sigmoid(a) * b).astype(BF16)
            return carry

        lax.fori_loop(0, n_exp, hidden, 0)
        if c == 0:
            for e in range(n_exp):
                down_weights(e).wait()

        def outputs(n, carry, c=c):
            acc = None
            cols = pl.ds(pl.multiple_of(n * COLS, COLS), COLS)
            for e in range(n_exp):
                o = jnp.dot(hid[e, :, :ff], w2[e, :, cols], preferred_element_type=F32) * gat[:, e:e + 1]
                acc = o if acc is None else acc + o
            part[c, n] = acc
            start_opposite(c, n)
            if c == 1:
                start_homeward(0, n)

                @pl.when(n >= 2)
                def _():
                    start_beside(1, n - 2)
            return carry

        lax.fori_loop(0, n_col, outputs, 0)

    for n in range(max(n_col - 2, 0), n_col):
        start_beside(1, n)
    for n in range(n_col):
        start_homeward(1, n)
    lane_k = lax.div(lax.broadcasted_iota(jnp.int32, (1, lanes), 1), blk)
    for n in range(n_col):
        steps = jnp.zeros((1, lanes), F32)
        for k in range(n_ep):
            if k:
                for r in homeward(k, n):
                    r.wait_recv()
            row = back_s[n, k]
            steps = jnp.where(lane_k == k, jnp.concatenate([row] * 2, axis=1), steps)
        y_ref[:, n * COLS:(n + 1) * COLS] = jnp.dot(
            st[...], _decode(back[n], steps), precision=lax.Precision.HIGHEST, preferred_element_type=F32).astype(BF16)

    for k in range(n_ep):
        if k:
            to_pos(k).wait_send()
        spread(k, 0).wait_send()
        spread(k, 1).wait_send()
        forward(k).wait_send()
        if k:
            for n in range(n_col):
                for r in homeward(k, n):
                    r.wait_send()
    for c in range(2):
        for n in range(n_col):
            for r in opposite(c, n) + beside(c, n):
                r.wait_send()


def solution(mesh):
    n_ep = mesh.shape['ep']
    rows_spec = P(('dp', 'ep', 'tp'), None)

    def body(x, idx, gate, w1, w3, w2):
        rows, width = x.shape
        n_exp, _, ff = w1.shape
        wide = ff // 256 * 256 - (-(ff % 256) // 128) * 128
        blk = 2 * rows // n_ep
        kl_n = n_ep // 2
        vrows, crows, n_col = kl_n * blk, 4 * kl_n * blk, width // COLS
        half = kl_n // 2 * blk
        dma = pltpu.SemaphoreType.DMA
        vmem = pl.BlockSpec(memory_space=pltpu.VMEM)
        anyw = pl.BlockSpec(memory_space=pl.ANY)
        return pl.pallas_call(
            functools.partial(_kernel, n_ep),
            out_shape=jax.ShapeDtypeStruct((rows, width), BF16),
            in_specs=[vmem] * 3 + [anyw] * 3,
            out_specs=vmem,
            scratch_shapes=[
                pltpu.VMEM((rows, n_ep * blk), F32),
                pltpu.VMEM((META, rows), F32),
                pltpu.VMEM((n_ep * blk, width + META), BF16),
                pltpu.VMEM((2 * crows, width + META), BF16),
                pltpu.VMEM((n_exp, 2 * wide, width), BF16),
                pltpu.VMEM(w2.shape, BF16),
                pltpu.VMEM((n_exp, crows, wide), BF16),
                pltpu.VMEM((crows, META), F32),
                pltpu.VMEM((2, n_col, crows, COLS), F32),
                pltpu.VMEM((n_col, n_ep * blk, COLS), I16),
                pltpu.VMEM((n_col, n_ep, 1, vrows), F32),
                pltpu.VMEM((2, n_col, vrows, COLS), I16),
                pltpu.VMEM((2, n_col, 1, vrows), F32),
                pltpu.VMEM((2, n_col, 2, half, COLS), I16),
                pltpu.VMEM((2, n_col, 2, 1, vrows), F32),
                pltpu.VMEM((2, n_col, 2, vrows, COLS), I16),
                pltpu.VMEM((2, n_col, 2, 1, vrows), F32),
                pltpu.VMEM((2, n_col, 2, vrows, COLS), I16),
                pltpu.VMEM((2, n_col, 2, 1, vrows), F32),
                pltpu.VMEM((2, n_col, vrows, COLS), I16),
                pltpu.VMEM((2, n_col, 1, vrows), F32),
                dma((5, n_exp)),
                dma((n_ep,)), dma((n_ep,)),
                dma((n_ep, 2)), dma((n_ep, 2)),
                dma((n_ep,)), dma((n_ep,)),
                dma((2, n_col, 2, 2)), dma((2, n_col, 2, 2)),
                dma((2, n_col, 2, 2)), dma((2, n_col, 2, 2)),
                dma((n_ep, n_col, 2)), dma((n_ep, n_col, 2)),
            ],
            compiler_params=pltpu.CompilerParams(
                collective_id=0, has_side_effects=True, vmem_limit_bytes=63 * 1024 * 1024),
        )(x, idx.T, gate.T, w1.swapaxes(1, 2), w3.swapaxes(1, 2), w2)

    return jax.shard_map(body, mesh=mesh,
                         in_specs=(rows_spec, rows_spec, rows_spec,
                                   P('ep', None, 'tp'), P('ep', None, 'tp'), P('ep', 'tp', None)),
                         out_specs=rows_spec, check_vma=False)
```

```python
import functools

import jax
import jax.numpy as jnp
from jax import lax
from jax.experimental import pallas as pl
from jax.experimental.pallas import tpu as pltpu
from jax.sharding import PartitionSpec as P

MESH = pl.DeviceIdType.MESH
F32, BF16, I16 = jnp.float32, jnp.bfloat16, jnp.int16
META = 128
COLS = 1024
STEPS = 32767.0
ROUND = 12582912.0


def _diagonal(n):
    return lax.broadcasted_iota(jnp.int32, (n, n), 0) == lax.broadcasted_iota(jnp.int32, (n, n), 1)


def _column(row, n):
    return jnp.sum(jnp.where(_diagonal(n), row, 0.0), axis=1, keepdims=True)


def _encode(val):
    n = val.shape[0]
    top = jnp.maximum(jnp.max(jnp.abs(val), axis=1, keepdims=True), 1e-33)
    code = (val * (STEPS / top) + ROUND) - ROUND
    step = jnp.sum(jnp.where(_diagonal(n), top * (1.0 / STEPS), 0.0), axis=0, keepdims=True)
    return code.astype(jnp.int32).astype(jnp.int16), step


def _decode(code, step):
    return code.astype(jnp.int32).astype(F32) * _column(step, code.shape[0])


def _kernel(n_ep, x_ref, idx_ref, gate_ref, w1_hbm, w3_hbm, w2_hbm, y_ref,
            st, mt, send, xr, w13, w2, hid, gat, part, back, back_s,
            far_o, far_os, near, near_s, side_o, side_os, full, full_s, home_o, home_os,
            w_sem, xs, xv, ys, yv, fs, fv, ns, nv, us, uv, bs, bv):
    rows, width = x_ref.shape
    top = idx_ref.shape[0]
    n_exp, ff, _ = w2.shape
    main = ff // 256 * 256
    rest = -(-(ff - main) // 128) * 128
    pad = main + rest - ff
    blk = 2 * rows // n_ep
    half_ep = n_ep // 2
    kl_n = n_ep // 2
    via = kl_n // 2
    vrows = kl_n * blk
    crows = 4 * vrows
    n_col = width // COLS

    p, t = lax.axis_index('ep'), lax.axis_index('tp')
    cx, cc = p // 2, p % 2
    up, dn = {'tp': (t + 1) % 4}, {'tp': (t + 3) % 4}

    def away(q):
        return q if q < 2 else half_ep + 1 - q

    def dest(k):
        return {'ep': 2 * ((cx + half_ep - away(k // 2)) % half_ep) + (cc + k % 2) % 2}

    def home(k):
        return {'ep': 2 * ((cx + away(k // 2)) % half_ep) + (cc + k % 2) % 2}

    def place(k, v):
        return pl.ds((k // kl_n) * crows + v * vrows + (k % kl_n) * blk, blk)

    def remote(src, dst, s, r, dev):
        return pltpu.make_async_remote_copy(src_ref=src, dst_ref=dst, send_sem=s, recv_sem=r,
                                            device_id=dev, device_id_type=MESH)

    def up_weights(e):
        parts = []
        for i, h in enumerate((w1_hbm, w3_hbm)):
            if main:
                parts.append((h.at[e, pl.ds(0, main)], w13.at[e, pl.ds(i * main, main)], w_sem.at[2 * i, e]))
            if rest:
                parts.append((h.at[e, pl.ds(main, ff - main)], w13.at[e, pl.ds(2 * main + i * rest, ff - main)],
                              w_sem.at[2 * i + 1, e]))
        return [pltpu.make_async_copy(*q) for q in parts]

    def down_weights(e):
        return pltpu.make_async_copy(w2_hbm.at[e], w2.at[e], w_sem.at[4, e])

    for e in range(n_exp):
        for c in up_weights(e):
            c.start()
    for e in range(n_exp):
        down_weights(e).start()

    barrier = pltpu.get_barrier_semaphore()
    for k in range(1, n_ep):
        pl.semaphore_signal(barrier, inc=1, device_id=dest(k), device_id_type=MESH)
    pl.semaphore_signal(barrier, inc=1, device_id=up, device_id_type=MESH)
    pl.semaphore_signal(barrier, inc=1, device_id=dn, device_id_type=MESH)

    idx = idx_ref[...]
    gate = gate_ref[...]
    lanes = n_ep * blk
    slot = lax.broadcasted_iota(jnp.int32, (lanes, rows), 0)
    kk = lax.div(slot, blk)
    q = lax.div(kk, 2)
    pos_of = 2 * lax.rem(cx + half_ep - jnp.where(q < 2, q, half_ep + 1 - q), half_ep) + lax.rem(cc + lax.rem(kk, 2), 2)
    first = pos_of * n_exp
    hit = jnp.zeros((lanes, rows), F32)
    for j in range(top):
        row = idx[j:j + 1]
        hit = jnp.where((row >= first) & (row < first + n_exp), 1.0, hit)
    before = jnp.where(lax.broadcasted_iota(jnp.int32, (rows, rows), 0) < lax.broadcasted_iota(jnp.int32, (rows, rows), 1),
                       1.0, 0.0)
    rank = jnp.dot(hit.astype(BF16), before.astype(BF16), preferred_element_type=F32)
    sel = jnp.where(rank == lax.rem(slot, blk).astype(F32), hit, 0.0)
    pick = sel.astype(BF16)

    g_hi = gate.astype(BF16).astype(F32)
    g_mid = (gate - g_hi).astype(BF16).astype(F32)
    mt[...] = jnp.zeros_like(mt)
    mt[0:top] = idx.astype(F32)
    mt[8:8 + top] = g_hi
    mt[16:16 + top] = g_mid
    mt[24:24 + top] = gate - g_hi - g_mid
    sent_meta = lax.dot_general(pick, mt[...].astype(BF16), (((1,), (1,)), ((), ())),
                                preferred_element_type=F32).astype(BF16)
    sent = jnp.dot(pick, x_ref[...], preferred_element_type=F32).astype(BF16)
    xr[:blk, :width] = sent[:blk]
    xr[:blk, width:] = sent_meta[:blk]
    send[:, :width] = sent
    send[:, width:] = sent_meta

    pl.semaphore_wait(barrier, n_ep + 1)

    def to_pos(k):
        return remote(send.at[pl.ds(k * blk, blk)], xr.at[place(k, 0)], xs.at[k], xv.at[k], dest(k))

    def spread(k, i):
        return remote(xr.at[place(k, 0)], xr.at[place(k, 1 if i else 3)], ys.at[k, i], yv.at[k, i], dn if i else up)

    def way(k):
        return 0 if k % kl_n < via else 1

    def forward(k):
        return remote(xr.at[place(k, 1 if way(k) else 3)], xr.at[place(k, 2)], fs.at[k], fv.at[k], dn if way(k) else up)

    def start_spread(k):
        if k:
            to_pos(k).wait_recv()
        spread(k, 0).start()
        spread(k, 1).start()

    def start_forward(k):
        spread(k, way(k)).wait_recv()
        forward(k).start()

    start_spread(0)
    for k in range(1, n_ep):
        to_pos(k).start()
    for k in range(1, kl_n):
        start_spread(k)
        start_forward(k - 1)
    start_forward(kl_n - 1)
    for k in range(kl_n, n_ep):
        start_spread(k)
    st[...] = sel.T
    if pad:
        for i in range(2):
            w13[:, pl.ds(2 * main + i * rest + rest - pad, pad)] = jnp.zeros((n_exp, pad, width), BF16)

    half = via * blk

    def opposite(c, n):
        out = []
        for i, rows_i, dev in ((0, pl.ds(0, half), up), (1, pl.ds(half, vrows - half), dn)):
            out.append(remote(far_o.at[c, n, rows_i], near.at[c, n, i], ns.at[c, n, i, 0], nv.at[c, n, i, 0], dev))
            out.append(remote(far_os.at[c, n], near_s.at[c, n, i], ns.at[c, n, i, 1], nv.at[c, n, i, 1], dev))
        return out

    def beside(c, n):
        out = []
        for i, dev in ((0, up), (1, dn)):
            out.append(remote(side_o.at[c, n, i], full.at[c, n, i], us.at[c, n, i, 0], uv.at[c, n, i, 0], dev))
            out.append(remote(side_os.at[c, n, i], full_s.at[c, n, i], us.at[c, n, i, 1], uv.at[c, n, i, 1], dev))
        return out

    def homeward(k, n):
        c = k // kl_n
        return [remote(home_o.at[c, n, pl.ds((k % kl_n) * blk, blk)], back.at[n, pl.ds(k * blk, blk)],
                       bs.at[k, n, 0], bv.at[k, n, 0], home(k)),
                remote(home_os.at[c, n], back_s.at[n, k], bs.at[k, n, 1], bv.at[k, n, 1], home(k))]

    def wait_all(copies):
        for r in copies:
            r.wait_recv()

    def start_all(copies):
        for r in copies:
            r.start()

    def make_opposite(c, n):
        far_o[c, n], far_os[c, n] = _encode(part[c, n, pl.ds(2 * vrows, vrows)])

    def make_beside(c, n):
        for i, at in ((0, 0), (1, half)):
            size = vrows - half if i else half
            more = _decode(near[c, n, i], near_s[c, n, i][:, at:at + size])
            mine = part[c, n, pl.ds((1, 3)[i] * vrows, vrows)]
            mine = jnp.concatenate([mine[:half], mine[half:] + more] if i else [mine[:half] + more, mine[half:]], axis=0)
            side_o[c, n, i], side_os[c, n, i] = _encode(mine)

    def make_homeward(c, n):
        total = part[c, n, pl.ds(0, vrows)]
        for i in range(2):
            total = total + _decode(full[c, n, i], full_s[c, n, i])
        code, step = _encode(total)
        home_o[c, n] = code
        home_os[c, n] = step
        if c == 0:
            back[n, pl.ds(0, blk)] = code[:blk]
            back_s[n, 0] = step

    def start_homeward(c, n):
        for k in range(max(c * kl_n, 1), (c + 1) * kl_n):
            start_all(homeward(k, n))

    def gather(c):
        for k in range(c * kl_n, (c + 1) * kl_n):
            spread(k, 1 - way(k)).wait_recv()
            forward(k).wait_recv()
        m = xr[pl.ds(c * crows, crows), width:].astype(F32)
        g_sum = m + pltpu.roll(m, META - 8, 1) + pltpu.roll(m, META - 16, 1)
        el = (lax.broadcasted_iota(jnp.int32, (crows, META), 1) + p * n_exp).astype(F32)
        g = jnp.zeros((crows, META), F32)
        for j in range(top):
            g = g + jnp.where(m[:, j:j + 1] == el, g_sum[:, 8 + j:9 + j], 0.0)
        gat[...] = g

    def hidden(c, e):
        ab = lax.dot_general(xr[pl.ds(c * crows, crows), :width], w13[e], (((1,), (1,)), ((), ())),
                             preferred_element_type=F32)
        for at, n in ((0, main), (2 * main, rest)):
            if n:
                a, b = ab[:, at:at + n], ab[:, at + n:at + 2 * n]
                hid[e, :, at // 2:at // 2 + n] = (a * jax.nn.sigmoid(a) * b).astype(BF16)

    def outputs(c, n, between):
        acc = None
        for e in range(n_exp):
            if e % 2 and between:
                between.pop(0)()
            o = jnp.dot(hid[e, :, :ff], w2[e, :, n * COLS:(n + 1) * COLS], preferred_element_type=F32) * gat[:, e:e + 1]
            acc = o if acc is None else acc + o
        for b in between:
            b()
        part[c, n] = acc

    gather(0)

    def first(e, carry):
        for w in up_weights(e):
            w.wait()
        for kl in range(kl_n - 1):
            @pl.when(e == 2 * kl + 2)
            def _():
                start_forward(kl_n + kl)
        hidden(0, e)
        return carry

    lax.fori_loop(0, n_exp, first, 0)
    start_forward(n_ep - 1)
    for e in range(n_exp):
        down_weights(e).wait()
    for n in range(n_col):
        outputs(0, n, [])
        make_opposite(0, n)
        start_all(opposite(0, n))

    gather(1)
    each = n_exp // n_col

    def second(n, carry):
        for i in range(each):
            if i == each // 2:
                wait_all(opposite(0, n))
                make_beside(0, n)
                start_all(beside(0, n))
            hidden(1, n * each + i)
        return carry

    lax.fori_loop(0, n_col, second, 0)
    last = n_col - 1
    for n in range(n_col):
        work = []
        if n:
            wait_all(beside(0, n - 1))
            work.append(lambda: make_homeward(0, n - 1))
        if n == last and n > 1:
            wait_all(opposite(1, 0))
            work.append(lambda: make_beside(1, 0))
        outputs(1, n, work)
        make_opposite(1, n)
        start_all(opposite(1, n))
        if n == last and n > 1:
            start_all(beside(1, 0))
        if n:
            start_homeward(0, n - 1)
    for n in range(1 if last > 1 else 0, n_col):
        if n == last:
            wait_all(beside(0, last))
            make_homeward(0, last)
            start_homeward(0, last)
        wait_all(opposite(1, n))
        make_beside(1, n)
        start_all(beside(1, n))
    for n in range(n_col):
        wait_all(beside(1, n))
        make_homeward(1, n)
        start_homeward(1, n)
    lane_k = lax.div(lax.broadcasted_iota(jnp.int32, (1, lanes), 1), blk)
    for n in range(n_col):
        steps = jnp.zeros((1, lanes), F32)
        for k in range(n_ep):
            if k:
                for r in homeward(k, n):
                    r.wait_recv()
            row = back_s[n, k]
            steps = jnp.where(lane_k == k, jnp.concatenate([row] * 2, axis=1), steps)
        y_ref[:, n * COLS:(n + 1) * COLS] = jnp.dot(
            st[...], _decode(back[n], steps), precision=lax.Precision.HIGHEST, preferred_element_type=F32).astype(BF16)

    for k in range(n_ep):
        if k:
            to_pos(k).wait_send()
        spread(k, 0).wait_send()
        spread(k, 1).wait_send()
        forward(k).wait_send()
        if k:
            for n in range(n_col):
                for r in homeward(k, n):
                    r.wait_send()
    for c in range(2):
        for n in range(n_col):
            for r in opposite(c, n) + beside(c, n):
                r.wait_send()


def solution(mesh):
    n_ep = mesh.shape['ep']
    rows_spec = P(('dp', 'ep', 'tp'), None)

    def body(x, idx, gate, w1, w3, w2):
        rows, width = x.shape
        n_exp, _, ff = w1.shape
        wide = ff // 256 * 256 - (-(ff % 256) // 128) * 128
        blk = 2 * rows // n_ep
        kl_n = n_ep // 2
        vrows, crows, n_col = kl_n * blk, 4 * kl_n * blk, width // COLS
        half = kl_n // 2 * blk
        dma = pltpu.SemaphoreType.DMA
        vmem = pl.BlockSpec(memory_space=pltpu.VMEM)
        anyw = pl.BlockSpec(memory_space=pl.ANY)
        return pl.pallas_call(
            functools.partial(_kernel, n_ep),
            out_shape=jax.ShapeDtypeStruct((rows, width), BF16),
            in_specs=[vmem] * 3 + [anyw] * 3,
            out_specs=vmem,
            scratch_shapes=[
                pltpu.VMEM((rows, n_ep * blk), F32),
                pltpu.VMEM((META, rows), F32),
                pltpu.VMEM((n_ep * blk, width + META), BF16),
                pltpu.VMEM((2 * crows, width + META), BF16),
                pltpu.VMEM((n_exp, 2 * wide, width), BF16),
                pltpu.VMEM(w2.shape, BF16),
                pltpu.VMEM((n_exp, crows, wide), BF16),
                pltpu.VMEM((crows, META), F32),
                pltpu.VMEM((2, n_col, crows, COLS), F32),
                pltpu.VMEM((n_col, n_ep * blk, COLS), I16),
                pltpu.VMEM((n_col, n_ep, 1, vrows), F32),
                pltpu.VMEM((2, n_col, vrows, COLS), I16),
                pltpu.VMEM((2, n_col, 1, vrows), F32),
                pltpu.VMEM((2, n_col, 2, half, COLS), I16),
                pltpu.VMEM((2, n_col, 2, 1, vrows), F32),
                pltpu.VMEM((2, n_col, 2, vrows, COLS), I16),
                pltpu.VMEM((2, n_col, 2, 1, vrows), F32),
                pltpu.VMEM((2, n_col, 2, vrows, COLS), I16),
                pltpu.VMEM((2, n_col, 2, 1, vrows), F32),
                pltpu.VMEM((2, n_col, vrows, COLS), I16),
                pltpu.VMEM((2, n_col, 1, vrows), F32),
                dma((5, n_exp)),
                dma((n_ep,)), dma((n_ep,)),
                dma((n_ep, 2)), dma((n_ep, 2)),
                dma((n_ep,)), dma((n_ep,)),
                dma((2, n_col, 2, 2)), dma((2, n_col, 2, 2)),
                dma((2, n_col, 2, 2)), dma((2, n_col, 2, 2)),
                dma((n_ep, n_col, 2)), dma((n_ep, n_col, 2)),
            ],
            compiler_params=pltpu.CompilerParams(
                collective_id=0, has_side_effects=True, vmem_limit_bytes=63 * 1024 * 1024),
        )(x, idx.T, gate.T, w1.swapaxes(1, 2), w3.swapaxes(1, 2), w2)

    return jax.shard_map(body, mesh=mesh,
                         in_specs=(rows_spec, rows_spec, rows_spec,
                                   P('ep', None, 'tp'), P('ep', None, 'tp'), P('ep', 'tp', None)),
                         out_specs=rows_spec, check_vma=False)
```

```python
import functools

import jax
import jax.numpy as jnp
from jax import lax
from jax.experimental import pallas as pl
from jax.experimental.pallas import tpu as pltpu
from jax.sharding import PartitionSpec as P

MESH = pl.DeviceIdType.MESH
F32, BF16, I16 = jnp.float32, jnp.bfloat16, jnp.int16
META = 128
COLS = 1024
STEPS = 32767.0
ROUND = 12582912.0


def _diagonal(n):
    return lax.broadcasted_iota(jnp.int32, (n, n), 0) == lax.broadcasted_iota(jnp.int32, (n, n), 1)


def _column(row, n):
    return jnp.sum(jnp.where(_diagonal(n), row, 0.0), axis=1, keepdims=True)


def _encode(val):
    n = val.shape[0]
    top = jnp.maximum(jnp.max(jnp.abs(val), axis=1, keepdims=True), 1e-33)
    code = (val * (STEPS / top) + ROUND) - ROUND
    step = jnp.sum(jnp.where(_diagonal(n), top * (1.0 / STEPS), 0.0), axis=0, keepdims=True)
    return code.astype(jnp.int32).astype(jnp.int16), step


def _decode(code, step):
    return code.astype(jnp.int32).astype(F32) * _column(step, code.shape[0])


def _kernel(n_ep, x_ref, idx_ref, gate_ref, w1_hbm, w3_hbm, w2_hbm, y_ref,
            st, mt, send, xr, w13, w2, hid, gat, part, back, back_s,
            far_o, far_os, near, near_s, side_o, side_os, full, full_s, home_o, home_os,
            w_sem, xs, xv, ys, yv, fs, fv, ns, nv, us, uv, bs, bv):
    rows, width = x_ref.shape
    top = idx_ref.shape[0]
    n_exp, ff, _ = w2.shape
    main = ff // 256 * 256
    rest = -(-(ff - main) // 128) * 128
    pad = main + rest - ff
    blk = 2 * rows // n_ep
    half_ep = n_ep // 2
    kl_n = n_ep // 2
    via = kl_n // 2
    vrows = kl_n * blk
    crows = 4 * vrows
    n_col = width // COLS

    p, t = lax.axis_index('ep'), lax.axis_index('tp')
    cx, cc = p // 2, p % 2
    up, dn = {'tp': (t + 1) % 4}, {'tp': (t + 3) % 4}

    def away(q):
        return q if q < 2 else half_ep + 1 - q

    def dest(k):
        return {'ep': 2 * ((cx + half_ep - away(k // 2)) % half_ep) + (cc + k % 2) % 2}

    def home(k):
        return {'ep': 2 * ((cx + away(k // 2)) % half_ep) + (cc + k % 2) % 2}

    def place(k, v):
        return pl.ds((k // kl_n) * crows + v * vrows + (k % kl_n) * blk, blk)

    def remote(src, dst, s, r, dev):
        return pltpu.make_async_remote_copy(src_ref=src, dst_ref=dst, send_sem=s, recv_sem=r,
                                            device_id=dev, device_id_type=MESH)

    def up_weights(e):
        parts = []
        for i, h in enumerate((w1_hbm, w3_hbm)):
            if main:
                parts.append((h.at[e, pl.ds(0, main)], w13.at[e, pl.ds(i * main, main)], w_sem.at[2 * i, e]))
            if rest:
                parts.append((h.at[e, pl.ds(main, ff - main)], w13.at[e, pl.ds(2 * main + i * rest, ff - main)],
                              w_sem.at[2 * i + 1, e]))
        return [pltpu.make_async_copy(*q) for q in parts]

    def down_weights(e):
        return pltpu.make_async_copy(w2_hbm.at[e], w2.at[e], w_sem.at[4, e])

    for e in range(n_exp):
        for c in up_weights(e):
            c.start()
    for e in range(n_exp):
        down_weights(e).start()

    barrier = pltpu.get_barrier_semaphore()
    for k in range(1, n_ep):
        pl.semaphore_signal(barrier, inc=1, device_id=dest(k), device_id_type=MESH)
    pl.semaphore_signal(barrier, inc=1, device_id=up, device_id_type=MESH)
    pl.semaphore_signal(barrier, inc=1, device_id=dn, device_id_type=MESH)

    idx = idx_ref[...]
    gate = gate_ref[...]
    lanes = n_ep * blk
    slot = lax.broadcasted_iota(jnp.int32, (lanes, rows), 0)
    kk = lax.div(slot, blk)
    q = lax.div(kk, 2)
    pos_of = 2 * lax.rem(cx + half_ep - jnp.where(q < 2, q, half_ep + 1 - q), half_ep) + lax.rem(cc + lax.rem(kk, 2), 2)
    first = pos_of * n_exp
    hit = jnp.zeros((lanes, rows), F32)
    for j in range(top):
        row = idx[j:j + 1]
        hit = jnp.where((row >= first) & (row < first + n_exp), 1.0, hit)
    before = jnp.where(lax.broadcasted_iota(jnp.int32, (rows, rows), 0) < lax.broadcasted_iota(jnp.int32, (rows, rows), 1),
                       1.0, 0.0)
    rank = jnp.dot(hit.astype(BF16), before.astype(BF16), preferred_element_type=F32)
    sel = jnp.where(rank == lax.rem(slot, blk).astype(F32), hit, 0.0)
    pick = sel.astype(BF16)

    g_hi = gate.astype(BF16).astype(F32)
    g_mid = (gate - g_hi).astype(BF16).astype(F32)
    mt[...] = jnp.zeros_like(mt)
    mt[0:top] = idx.astype(F32)
    mt[8:8 + top] = g_hi
    mt[16:16 + top] = g_mid
    mt[24:24 + top] = gate - g_hi - g_mid
    sent_meta = lax.dot_general(pick, mt[...].astype(BF16), (((1,), (1,)), ((), ())),
                                preferred_element_type=F32).astype(BF16)
    sent = jnp.dot(pick, x_ref[...], preferred_element_type=F32).astype(BF16)
    xr[:blk, :width] = sent[:blk]
    xr[:blk, width:] = sent_meta[:blk]
    send[:, :width] = sent
    send[:, width:] = sent_meta

    pl.semaphore_wait(barrier, n_ep + 1)

    def to_pos(k):
        return remote(send.at[pl.ds(k * blk, blk)], xr.at[place(k, 0)], xs.at[k], xv.at[k], dest(k))

    def spread(k, i):
        return remote(xr.at[place(k, 0)], xr.at[place(k, 1 if i else 3)], ys.at[k, i], yv.at[k, i], dn if i else up)

    def way(k):
        return 0 if k % kl_n < via else 1

    def forward(k):
        return remote(xr.at[place(k, 1 if way(k) else 3)], xr.at[place(k, 2)], fs.at[k], fv.at[k], dn if way(k) else up)

    def late(v, lo, hi):
        return xr.at[pl.ds(crows + v * vrows + lo, hi - lo)]

    def spread_late(i):
        return remote(late(0, 0, vrows), late(1 if i else 3, 0, vrows), ys.at[kl_n, i], yv.at[kl_n, i], dn if i else up)

    def forward_late(i):
        lo, hi = (via * blk, vrows) if i else (0, via * blk)
        return remote(late(1 if i else 3, lo, hi), late(2, lo, hi), fs.at[kl_n + i], fv.at[kl_n + i], dn if i else up)

    def start_spread(k):
        if k:
            to_pos(k).wait_recv()
        spread(k, 0).start()
        spread(k, 1).start()

    def start_forward(k):
        spread(k, way(k)).wait_recv()
        forward(k).start()

    start_spread(0)
    for k in range(1, n_ep):
        to_pos(k).start()
    for k in range(1, kl_n):
        start_spread(k)
        start_forward(k - 1)
    start_forward(kl_n - 1)
    for k in range(kl_n, n_ep):
        to_pos(k).wait_recv()
    for i in range(2):
        spread_late(i).start()
    st[...] = sel.T
    if pad:
        for i in range(2):
            w13[:, pl.ds(2 * main + i * rest + rest - pad, pad)] = jnp.zeros((n_exp, pad, width), BF16)

    half = via * blk

    def opposite(c, n):
        out = []
        for i, rows_i, dev in ((0, pl.ds(0, half), up), (1, pl.ds(half, vrows - half), dn)):
            out.append(remote(far_o.at[c, n, rows_i], near.at[c, n, i], ns.at[c, n, i, 0], nv.at[c, n, i, 0], dev))
            out.append(remote(far_os.at[c, n], near_s.at[c, n, i], ns.at[c, n, i, 1], nv.at[c, n, i, 1], dev))
        return out

    def beside(c, n):
        out = []
        for i, dev in ((0, up), (1, dn)):
            out.append(remote(side_o.at[c, n, i], full.at[c, n, i], us.at[c, n, i, 0], uv.at[c, n, i, 0], dev))
            out.append(remote(side_os.at[c, n, i], full_s.at[c, n, i], us.at[c, n, i, 1], uv.at[c, n, i, 1], dev))
        return out

    def homeward(k, n):
        c = k // kl_n
        return [remote(home_o.at[c, n, pl.ds((k % kl_n) * blk, blk)], back.at[n, pl.ds(k * blk, blk)],
                       bs.at[k, n, 0], bv.at[k, n, 0], home(k)),
                remote(home_os.at[c, n], back_s.at[n, k], bs.at[k, n, 1], bv.at[k, n, 1], home(k))]

    def wait_all(copies):
        for r in copies:
            r.wait_recv()

    def start_all(copies):
        for r in copies:
            r.start()

    def make_opposite(c, n):
        far_o[c, n], far_os[c, n] = _encode(part[c, n, pl.ds(2 * vrows, vrows)])

    def make_beside(c, n):
        for i, at in ((0, 0), (1, half)):
            size = vrows - half if i else half
            more = _decode(near[c, n, i], near_s[c, n, i][:, at:at + size])
            mine = part[c, n, pl.ds((1, 3)[i] * vrows, vrows)]
            mine = jnp.concatenate([mine[:half], mine[half:] + more] if i else [mine[:half] + more, mine[half:]], axis=0)
            side_o[c, n, i], side_os[c, n, i] = _encode(mine)

    def make_homeward(c, n):
        total = part[c, n, pl.ds(0, vrows)]
        for i in range(2):
            total = total + _decode(full[c, n, i], full_s[c, n, i])
        code, step = _encode(total)
        home_o[c, n] = code
        home_os[c, n] = step
        if c == 0:
            back[n, pl.ds(0, blk)] = code[:blk]
            back_s[n, 0] = step

    def start_homeward(c, n):
        for k in range(max(c * kl_n, 1), (c + 1) * kl_n):
            start_all(homeward(k, n))

    def gather(c):
        for k in range(0 if c else kl_n):
            spread(k, 1 - way(k)).wait_recv()
            forward(k).wait_recv()
        for i in range(2 if c else 0):
            forward_late(i).wait_recv()
        m = xr[pl.ds(c * crows, crows), width:].astype(F32)
        g_sum = m + pltpu.roll(m, META - 8, 1) + pltpu.roll(m, META - 16, 1)
        el = (lax.broadcasted_iota(jnp.int32, (crows, META), 1) + p * n_exp).astype(F32)
        g = jnp.zeros((crows, META), F32)
        for j in range(top):
            g = g + jnp.where(m[:, j:j + 1] == el, g_sum[:, 8 + j:9 + j], 0.0)
        gat[...] = g

    def hidden(c, e):
        ab = lax.dot_general(xr[pl.ds(c * crows, crows), :width], w13[e], (((1,), (1,)), ((), ())),
                             preferred_element_type=F32)
        for at, n in ((0, main), (2 * main, rest)):
            if n:
                a, b = ab[:, at:at + n], ab[:, at + n:at + 2 * n]
                hid[e, :, at // 2:at // 2 + n] = (a * jax.nn.sigmoid(a) * b).astype(BF16)

    def outputs(c, n, between):
        acc = None
        for e in range(n_exp):
            if e % 2 and between:
                between.pop(0)()
            o = jnp.dot(hid[e, :, :ff], w2[e, :, n * COLS:(n + 1) * COLS], preferred_element_type=F32) * gat[:, e:e + 1]
            acc = o if acc is None else acc + o
        for b in between:
            b()
        part[c, n] = acc

    gather(0)

    def first(e, carry):
        for w in up_weights(e):
            w.wait()
        @pl.when(e == n_exp - 3)
        def _():
            for i in range(2):
                spread_late(i).wait_recv()
                forward_late(i).start()

        hidden(0, e)
        return carry

    lax.fori_loop(0, n_exp, first, 0)
    for e in range(n_exp):
        down_weights(e).wait()
    for n in range(n_col):
        outputs(0, n, [])
        make_opposite(0, n)
        start_all(opposite(0, n))

    gather(1)
    each = n_exp // n_col

    def second(n, carry):
        for i in range(each):
            if i == each // 2:
                wait_all(opposite(0, n))
                make_beside(0, n)
                start_all(beside(0, n))
            hidden(1, n * each + i)
        return carry

    lax.fori_loop(0, n_col, second, 0)
    last = n_col - 1
    for n in range(n_col):
        work = []
        if n:
            wait_all(beside(0, n - 1))
            work.append(lambda: make_homeward(0, n - 1))
        if n == last and n > 1:
            wait_all(opposite(1, 0))
            work.append(lambda: make_beside(1, 0))
        outputs(1, n, work)
        make_opposite(1, n)
        start_all(opposite(1, n))
        if n == last and n > 1:
            start_all(beside(1, 0))
        if n:
            start_homeward(0, n - 1)
    for n in range(1 if last > 1 else 0, n_col):
        if n == last:
            wait_all(beside(0, last))
            make_homeward(0, last)
            start_homeward(0, last)
        wait_all(opposite(1, n))
        make_beside(1, n)
        start_all(beside(1, n))
    for n in range(n_col):
        wait_all(beside(1, n))
        make_homeward(1, n)
        start_homeward(1, n)
    lane_k = lax.div(lax.broadcasted_iota(jnp.int32, (1, lanes), 1), blk)
    for n in range(n_col):
        steps = jnp.zeros((1, lanes), F32)
        for k in range(n_ep):
            if k:
                for r in homeward(k, n):
                    r.wait_recv()
            row = back_s[n, k]
            steps = jnp.where(lane_k == k, jnp.concatenate([row] * 2, axis=1), steps)
        y_ref[:, n * COLS:(n + 1) * COLS] = jnp.dot(
            st[...], _decode(back[n], steps), precision=lax.Precision.HIGHEST, preferred_element_type=F32).astype(BF16)

    for k in range(n_ep):
        if k:
            to_pos(k).wait_send()
        if k < kl_n:
            spread(k, 0).wait_send()
            spread(k, 1).wait_send()
            forward(k).wait_send()
        if k:
            for n in range(n_col):
                for r in homeward(k, n):
                    r.wait_send()
    for i in range(2):
        spread_late(i).wait_send()
        forward_late(i).wait_send()
    for c in range(2):
        for n in range(n_col):
            for r in opposite(c, n) + beside(c, n):
                r.wait_send()


def solution(mesh):
    n_ep = mesh.shape['ep']
    rows_spec = P(('dp', 'ep', 'tp'), None)

    def body(x, idx, gate, w1, w3, w2):
        rows, width = x.shape
        n_exp, _, ff = w1.shape
        wide = ff // 256 * 256 - (-(ff % 256) // 128) * 128
        blk = 2 * rows // n_ep
        kl_n = n_ep // 2
        vrows, crows, n_col = kl_n * blk, 4 * kl_n * blk, width // COLS
        half = kl_n // 2 * blk
        dma = pltpu.SemaphoreType.DMA
        vmem = pl.BlockSpec(memory_space=pltpu.VMEM)
        anyw = pl.BlockSpec(memory_space=pl.ANY)
        return pl.pallas_call(
            functools.partial(_kernel, n_ep),
            out_shape=jax.ShapeDtypeStruct((rows, width), BF16),
            in_specs=[vmem] * 3 + [anyw] * 3,
            out_specs=vmem,
            scratch_shapes=[
                pltpu.VMEM((rows, n_ep * blk), F32),
                pltpu.VMEM((META, rows), F32),
                pltpu.VMEM((n_ep * blk, width + META), BF16),
                pltpu.VMEM((2 * crows, width + META), BF16),
                pltpu.VMEM((n_exp, 2 * wide, width), BF16),
                pltpu.VMEM(w2.shape, BF16),
                pltpu.VMEM((n_exp, crows, wide), BF16),
                pltpu.VMEM((crows, META), F32),
                pltpu.VMEM((2, n_col, crows, COLS), F32),
                pltpu.VMEM((n_col, n_ep * blk, COLS), I16),
                pltpu.VMEM((n_col, n_ep, 1, vrows), F32),
                pltpu.VMEM((2, n_col, vrows, COLS), I16),
                pltpu.VMEM((2, n_col, 1, vrows), F32),
                pltpu.VMEM((2, n_col, 2, half, COLS), I16),
                pltpu.VMEM((2, n_col, 2, 1, vrows), F32),
                pltpu.VMEM((2, n_col, 2, vrows, COLS), I16),
                pltpu.VMEM((2, n_col, 2, 1, vrows), F32),
                pltpu.VMEM((2, n_col, 2, vrows, COLS), I16),
                pltpu.VMEM((2, n_col, 2, 1, vrows), F32),
                pltpu.VMEM((2, n_col, vrows, COLS), I16),
                pltpu.VMEM((2, n_col, 1, vrows), F32),
                dma((5, n_exp)),
                dma((n_ep,)), dma((n_ep,)),
                dma((n_ep, 2)), dma((n_ep, 2)),
                dma((n_ep,)), dma((n_ep,)),
                dma((2, n_col, 2, 2)), dma((2, n_col, 2, 2)),
                dma((2, n_col, 2, 2)), dma((2, n_col, 2, 2)),
                dma((n_ep, n_col, 2)), dma((n_ep, n_col, 2)),
            ],
            compiler_params=pltpu.CompilerParams(
                collective_id=0, has_side_effects=True, vmem_limit_bytes=63 * 1024 * 1024),
        )(x, idx.T, gate.T, w1.swapaxes(1, 2), w3.swapaxes(1, 2), w2)

    return jax.shard_map(body, mesh=mesh,
                         in_specs=(rows_spec, rows_spec, rows_spec,
                                   P('ep', None, 'tp'), P('ep', None, 'tp'), P('ep', 'tp', None)),
                         out_specs=rows_spec, check_vma=False)
```
